64 devices in a mesh: rep: 4 (over x, y), dp: 16 (over z, core).
Axes of the slice: x: 2, y: 2, z: 8, core: 2. Of those that a mesh axis runs over, the one named last changes fastest.
The devices are a block of a 4x4x8 slice.
Arguments:
- x: bfloat16 [64, 1024, 640], P(('rep', 'dp')), parts along dimension 0
- dy: bfloat16 [64, 1024, 640], P(('rep', 'dp')), parts along dimension 0
- wq: bfloat16 [2, 640, 640], P(None, 'dp')
- wk: bfloat16 [2, 640, 128], P(None, 'dp')
- wv: bfloat16 [2, 640, 128], P(None, 'dp')
- wo: bfloat16 [2, 640, 640], P(None, 'dp')
- w_gate: bfloat16 [2, 640, 2048], P(None, 'dp')
- w_up: bfloat16 [2, 640, 2048], P(None, 'dp')
- w_down: bfloat16 [2, 2048, 640], P(None, 'dp')
- m_wq: float32 [2, 640, 640], P(None, 'dp')
- m_wk: float32 [2, 640, 128], P(None, 'dp')
- m_wv: float32 [2, 640, 128], P(None, 'dp')
- m_wo: float32 [2, 640, 640], P(None, 'dp')
- m_w_gate: float32 [2, 640, 2048], P(None, 'dp')
- m_w_up: float32 [2, 640, 2048], P(None, 'dp')
- m_w_down: float32 [2, 2048, 640], P(None, 'dp')
- v_wq: float32 [2, 640, 640], P(None, 'dp')
- v_wk: float32 [2, 640, 128], P(None, 'dp')
- v_wv: float32 [2, 640, 128], P(None, 'dp')
- v_wo: float32 [2, 640, 640], P(None, 'dp')
- v_w_gate: float32 [2, 640, 2048], P(None, 'dp')
- v_w_up: float32 [2, 640, 2048], P(None, 'dp')
- v_w_down: float32 [2, 2048, 640], P(None, 'dp')
Outputs:
- output 1: bfloat16 [8, 640, 640], P('rep', 'dp'), parts along dimension 0
- output 2: bfloat16 [8, 640, 128], P('rep', 'dp'), parts along dimension 0
- output 3: bfloat16 [8, 640, 128], P('rep', 'dp'), parts along dimension 0
- output 4: bfloat16 [8, 640, 640], P('rep', 'dp'), parts along dimension 0
- output 5: bfloat16 [8, 640, 2048], P('rep', 'dp'), parts along dimension 0
- output 6: bfloat16 [8, 640, 2048], P('rep', 'dp'), parts along dimension 0
- output 7: bfloat16 [8, 2048, 640], P('rep', 'dp'), parts along dimension 0
- output 8: float32 [8, 640, 640], P('rep', 'dp'), parts along dimension 0
- output 9: float32 [8, 640, 128], P('rep', 'dp'), parts along dimension 0
- output 10: float32 [8, 640, 128], P('rep', 'dp'), parts along dimension 0
- output 11: float32 [8, 640, 640], P('rep', 'dp'), parts along dimension 0
- output 12: float32 [8, 640, 2048], P('rep', 'dp'), parts along dimension 0
- output 13: float32 [8, 640, 2048], P('rep', 'dp'), parts along dimension 0
- output 14: float32 [8, 2048, 640], P('rep', 'dp'), parts along dimension 0
- output 15: float32 [8, 640, 640], P('rep', 'dp'), parts along dimension 0
- output 16: float32 [8, 640, 128], P('rep', 'dp'), parts along dimension 0
- output 17: float32 [8, 640, 128], P('rep', 'dp'), parts along dimension 0
- output 18: float32 [8, 640, 640], P('rep', 'dp'), parts along dimension 0
- output 19: float32 [8, 640, 2048], P('rep', 'dp'), parts along dimension 0
- output 20: float32 [8, 640, 2048], P('rep', 'dp'), parts along dimension 0
- output 21: float32 [8, 2048, 640], P('rep', 'dp'), parts along dimension 0
There are 4 independent parts. The reference program is written for one: setup_inputs(seed, part) draws one part's arguments, and reference() takes and returns one part's arrays. A program takes and returns all parts, laid end to end along the dimension named above; an argument that names none is the same for every part.
All inputs are finite; a program needn't handle non-finite values.
Results may differ from the reference program's by a relative error of at most 0.0258.
Values are sent between devices in bfloat16 or wider.
A program may use at most 768 MiB of HBM per device.

```python
import jax
import jax.numpy as jnp
from jax import lax

SEQUENCES = 16
TOKENS = 1024
D = 640
HEADS = 5
KV_HEADS = 1
HEAD = 128
FF = 2048
LAYERS = 2
THETA = 10000
NAMES = ("wq", "wk", "wv", "wo", "w_gate", "w_up", "w_down")
SHAPES = {
    "wq": (LAYERS, D, HEADS * HEAD),
    "wk": (LAYERS, D, KV_HEADS * HEAD),
    "wv": (LAYERS, D, KV_HEADS * HEAD),
    "wo": (LAYERS, HEADS * HEAD, D),
    "w_gate": (LAYERS, D, FF),
    "w_up": (LAYERS, D, FF),
    "w_down": (LAYERS, FF, D),
}


def bump(key, n, height):
    away = (jnp.arange(n, dtype=jnp.int32) - jax.random.randint(key, (), 0, n, jnp.int32)) % n
    return jnp.where(away < n // 8, height, 1.0)


def together(key, own, strength):
    shared = jax.random.normal(key, own.shape[1:], jnp.float32)
    return (own + strength * shared) * lax.rsqrt(1 + strength * strength)


def setup_inputs(seed: int = 0, part: int = 0) -> dict:
    kx, kdy, ka, kb, kz, kf, kh, kl, *keys = jax.random.split(jax.random.key(seed), 8 + 3 * len(NAMES))
    kx, kdy, ka, kb = (jax.random.fold_in(k, part) for k in (kx, kdy, ka, kb))
    kw, km, kv = (keys[i::3] for i in range(3))
    shape = (SEQUENCES, TOKENS, D)
    much_x, much_dy = jax.random.uniform(kz, (2,), jnp.float32, 0.0, 1.0)
    loud = 2.0 ** jax.random.uniform(jax.random.fold_in(kz, 1), (), jnp.float32, -1.0, 2.0)
    layers = 2.0 ** jax.random.uniform(kl, (LAYERS, 1, 1), jnp.float32, -1.0, 1.0)
    times = {"wq": 1.0, "wk": 1.0, "wv": 2.0, "wo": layers, "w_gate": 1.0, "w_up": bump(kh, FF, 4.0), "w_down": layers}
    x = together(ka, jax.random.normal(kx, shape, jnp.float32), much_x) * bump(kf, D, 4.0)
    dy = together(kb, jax.random.normal(kdy, shape, jnp.float32), much_dy)
    drawn = {"x": x.astype(jnp.bfloat16), "dy": (loud * dy * (SEQUENCES * TOKENS) ** -0.5).astype(jnp.bfloat16)}
    for key, name in zip(kw, NAMES, strict=True):
        drawn[name] = (jax.random.normal(key, SHAPES[name], jnp.float32) * SHAPES[name][1] ** -0.5 * times[name]).astype(jnp.bfloat16)
    for key, name in zip(km, NAMES, strict=True):
        drawn[f"m_{name}"] = 0.1 * jax.random.normal(key, SHAPES[name], jnp.float32)
    for key, name in zip(kv, NAMES, strict=True):
        drawn[f"v_{name}"] = jax.random.uniform(key, SHAPES[name], jnp.float32, 0.02, 0.06)
    return drawn


def matmul(a, w):
    return jnp.dot(a, w, preferred_element_type=jnp.float32).astype(jnp.bfloat16)


def normed(h):
    wide = h.astype(jnp.float32)
    scale = lax.rsqrt(jnp.mean(wide**2, -1, keepdims=True) + 1e-6)
    return (wide * scale).astype(jnp.bfloat16)


def turned(t, theta):
    half = t.shape[-1] // 2
    angle = jnp.arange(t.shape[0], dtype=jnp.float32)[:, None] * theta ** (-jnp.arange(half, dtype=jnp.float32) / half)
    cos, sin = jnp.cos(angle)[:, None], jnp.sin(angle)[:, None]
    a, b = t[..., :half].astype(jnp.float32), t[..., half:].astype(jnp.float32)
    return jnp.concatenate([a * cos - b * sin, b * cos + a * sin], -1).astype(jnp.bfloat16)


def seen_by(q, k, v):
    tokens, kv = q.shape[0], k.shape[1]
    q = q.reshape(tokens, kv, -1, q.shape[-1])
    scores = jnp.einsum("tgsd,ugd->gstu", q.astype(jnp.float32), k.astype(jnp.float32)) * q.shape[-1] ** -0.5
    place = jnp.arange(tokens)
    weights = jax.nn.softmax(jnp.where(place[:, None] >= place, scores, -jnp.inf), -1).astype(jnp.bfloat16)
    return jnp.einsum("gstu,ugd->tgsd", weights.astype(jnp.float32), v.astype(jnp.float32)).astype(jnp.bfloat16).reshape(tokens, -1)


def layer(h, w):
    a = normed(h)
    q, k = (turned(matmul(a, w[name]).reshape(h.shape[0], -1, HEAD), THETA) for name in ("wq", "wk"))
    h = h + matmul(seen_by(q, k, matmul(a, w["wv"]).reshape(h.shape[0], -1, HEAD)), w["wo"])
    b = normed(h)
    gate = jnp.dot(b, w["w_gate"], preferred_element_type=jnp.float32)
    up = jnp.dot(b, w["w_up"], preferred_element_type=jnp.float32)
    return h + matmul((jax.nn.silu(gate) * up).astype(jnp.bfloat16), w["w_down"])


def adamw(w, m, v, g):
    m = 0.9 * m + 0.1 * g
    v = 0.95 * v + 0.05 * g * g
    step = m * lax.rsqrt(v + 1e-8) + 0.1 * w
    return (w - 0.02 * step).astype(jnp.bfloat16), m, v


def clipped(gradients, sum_of_squares, count):
    factor = jnp.minimum(1.0, 0.5 * lax.rsqrt(sum_of_squares / count + 1e-30))
    return [g * factor for g in gradients]


def stack(weights, h):
    return lax.scan(lambda h, w: (layer(h, w), None), h, weights)[0]


def reference(x, dy, wq, wk, wv, wo, w_gate, w_up, w_down, m_wq, m_wk, m_wv, m_wo, m_w_gate, m_w_up, m_w_down, v_wq, v_wk, v_wv, v_wo, v_w_gate, v_w_up, v_w_down):
    weights = dict(zip(NAMES, (wq, wk, wv, wo, w_gate, w_up, w_down), strict=True))

    def take(so_far, sequence):
        h, by_y = sequence
        _, back = jax.vjp(stack, weights, h)
        by_weights, by_h = back(by_y)
        return jax.tree.map(lambda total, term: total + term.astype(jnp.float32), so_far, by_weights), by_h

    none_yet = {name: jnp.zeros(w.shape, jnp.float32) for name, w in weights.items()}
    by_weights, by_x = lax.scan(take, none_yet, (x, dy))
    gradients = [by_weights[name].astype(jnp.bfloat16).astype(jnp.float32) for name in NAMES]
    gradients = clipped(gradients, sum(jnp.sum(g * g) for g in gradients), sum(g.size for g in gradients))
    first = (m_wq, m_wk, m_wv, m_wo, m_w_gate, m_w_up, m_w_down)
    second = (v_wq, v_wk, v_wv, v_wo, v_w_gate, v_w_up, v_w_down)
    new = [adamw(weights[name].astype(jnp.float32), m, v, g) for name, m, v, g in zip(NAMES, first, second, gradients, strict=True)]
    return tuple(one[which] for which in range(3) for one in new)
```

```python
import functools

import jax
import jax.numpy as jnp
from jax import lax
from jax.experimental import pallas as pl
from jax.experimental.pallas import tpu as pltpu
from jax.sharding import PartitionSpec as P

NEG = -1e30
HIDDEN = 2 * NEG
LOG2E = 1.4426950408889634
VMEM = 56 * 2**20
STRIP = 512
BQ = 512


def _dot(a, b, ca, cb):
    return lax.dot_general(a, b, (((ca,), (cb,)), ((), ())), preferred_element_type=jnp.float32)


def _gap(bk, cols, bq):
    return lax.rem(lax.broadcasted_iota(jnp.int32, (bk, cols), 1), bq) - lax.broadcasted_iota(jnp.int32, (bk, cols), 0)


def _row(ref):
    return jnp.concatenate([ref[i : i + 1, :] for i in range(ref.shape[0])], axis=1)


def _over_keys(block, iq, bq, bk):
    whole, last = lax.div(iq * bq, bk), lax.div(iq * bq + bq, bk)
    lax.fori_loop(0, whole, lambda j, _: block(j, False), None)
    lax.fori_loop(whole, last, lambda j, _: block(j, True), None)


def _forward(q_ref, k_ref, v_ref, o_ref, lse_ref, top_s, mix_s, gap_s, *, bk):
    g, bq, d = q_ref.shape
    cols, low = g * bq, k_ref.dtype
    iq = pl.program_id(0)
    scale = d**-0.5
    e = scale * LOG2E
    pieces = range(0, cols, STRIP)

    @pl.when(iq == 0)
    def _():
        gap_s[...] = _gap(bk, cols, bq)

    top_s[...] = jnp.full(top_s.shape, NEG, jnp.float32)
    mix_s[...] = jnp.zeros(mix_s.shape, jnp.float32)
    ones = jnp.ones((8, bk), low)

    def block(j, masked):
        here = pl.ds(pl.multiple_of(j * bk, bk), bk)
        scores = [_dot(k_ref[here, :], q_ref[...].reshape(cols, d)[at : at + STRIP, :], 1, 1) for at in pieces]
        weights, keeps = [], []
        for at, s in zip(pieces, scores):
            if masked:
                s = jnp.where(gap_s[:, at : at + STRIP] >= j * bk - iq * bq, s, HIDDEN)
            old = top_s[:, at : at + STRIP]
            top = jnp.maximum(old, s.max(axis=0, keepdims=True))
            top_s[:, at : at + STRIP] = top
            weights.append(jnp.exp2((s - top) * e).astype(low))
            keeps.append(jnp.exp2((old - top) * e))
        values = jnp.concatenate([v_ref[here, :].T, ones], axis=0)
        for at, p, keep in zip(pieces, weights, keeps):
            mix_s[:, at : at + STRIP] = mix_s[:, at : at + STRIP] * keep + _dot(values, p, 1, 0)

    _over_keys(block, iq, bq, bk)
    total = mix_s[d : d + 1, :]
    o_ref[...] = (mix_s[:d, :] * (1 / total)).T.reshape(g, bq, d).astype(o_ref.dtype)
    lse = top_s[...] * scale + jnp.log(total)
    for i in range(g):
        lse_ref[i : i + 1, :] = lse[:, i * bq : (i + 1) * bq]


def _backward(q_ref, k_ref, v_ref, do_ref, lse_ref, delta_ref, dq_ref, dk_ref, dv_ref, dq_s, dk_s, dv_s, gap_s, *, bk):
    g, bq, d = q_ref.shape
    cols, low = g * bq, q_ref.dtype
    iq = pl.program_id(0)
    scale = d**-0.5
    e = scale * LOG2E
    pieces = range(0, cols, STRIP)

    @pl.when(iq == 0)
    def _():
        gap_s[...] = _gap(bk, cols, bq)
        dk_s[...] = jnp.zeros_like(dk_s)
        dv_s[...] = jnp.zeros_like(dv_s)

    dq_s[...] = jnp.zeros_like(dq_s)
    lses, deltas = _row(lse_ref) * LOG2E, _row(delta_ref)

    def block(j, masked):
        here = pl.ds(pl.multiple_of(j * bk, bk), bk)
        qs = [q_ref[...].reshape(cols, d)[at : at + STRIP, :] for at in pieces]
        dos = [do_ref[...].reshape(cols, d)[at : at + STRIP, :] for at in pieces]
        scores = [_dot(k_ref[here, :], one, 1, 1) for one in qs]
        dps = [_dot(v_ref[here, :], one, 1, 1) for one in dos]
        for at, q, do, s, dp in zip(pieces, qs, dos, scores, dps):
            p = jnp.exp2(s * e - lses[:, at : at + STRIP])
            if masked:
                p = jnp.where(gap_s[:, at : at + STRIP] >= j * bk - iq * bq, p, 0.0)
            ds = (p * (dp - deltas[:, at : at + STRIP])).astype(low)
            dv_s[here, :] += _dot(p.astype(low), do, 1, 0)
            dk_s[here, :] += _dot(ds, q, 1, 0)
            dq_s[:, at : at + STRIP] += _dot(k_ref[here, :].T, ds, 1, 0)

    _over_keys(block, iq, bq, bk)
    dq_ref[...] = (dq_s[...] * scale).T.reshape(g, bq, d).astype(dq_ref.dtype)

    @pl.when(iq == pl.num_programs(0) - 1)
    def _():
        dk_ref[...] = (dk_s[...] * scale).astype(dk_ref.dtype)
        dv_ref[...] = dv_s[...].astype(dv_ref.dtype)


def _specs(q):
    g, tokens, d = q.shape
    return (pl.BlockSpec((g, BQ, d), lambda iq: (0, iq, 0)), pl.BlockSpec((tokens, d), lambda iq: (0, 0)),
            pl.BlockSpec((g, BQ), lambda iq: (0, iq)))


def _params():
    return pltpu.CompilerParams(vmem_limit_bytes=VMEM, dimension_semantics=("arbitrary",))


def attend(q, k, v):
    g, tokens, d = q.shape
    queries, keys, stats = _specs(q)
    bk, cols = BQ // 2, g * BQ
    return pl.pallas_call(
        functools.partial(_forward, bk=bk), name="attend", grid=(tokens // BQ,), in_specs=[queries, keys, keys], out_specs=[queries, stats],
        out_shape=[_like(*q.shape), _like(g, tokens, dtype=F32)],
        scratch_shapes=[pltpu.VMEM((1, cols), F32), pltpu.VMEM((d + 8, cols), F32), pltpu.VMEM((bk, cols), jnp.int32)],
        compiler_params=_params(), cost_estimate=_price(4 * g * tokens * tokens * d, q, q, k, v))(q, k, v)


def attend_bwd(q, k, v, do, lse, delta):
    g, tokens, d = q.shape
    queries, keys, stats = _specs(q)
    bk, cols = BQ // 2, g * BQ
    return pl.pallas_call(
        functools.partial(_backward, bk=bk), name="attend_back", grid=(tokens // BQ,),
        in_specs=[queries, keys, keys, queries, stats, stats], out_specs=[queries, keys, keys],
        out_shape=[_like(*q.shape), _like(*k.shape), _like(*v.shape)],
        scratch_shapes=[pltpu.VMEM((d, cols), F32), pltpu.VMEM((tokens, d), F32), pltpu.VMEM((tokens, d), F32),
                        pltpu.VMEM((bk, cols), jnp.int32)],
        compiler_params=_params(), cost_estimate=_price(10 * g * tokens * tokens * d, q, q, q, k, v))(q, k, v, do, lse, delta)


HEAD = 128
THETA = 10000
NAMES = ("wq", "wk", "wv", "wo", "w_gate", "w_up", "w_down")
BF, F32 = jnp.bfloat16, jnp.float32
TILE = 512
ROWS = 512
MESH = pl.DeviceIdType.MESH


def packed_down(w):
    u, d = w.shape
    return w.reshape(u // 8, 8, d // 128, 128).transpose(2, 1, 0, 3).reshape(d // 16, 16 * u)


def unpacked_down(p):
    d, u = p.shape[0] * 16, p.shape[1] // 16
    return p.reshape(d // 128, 8, u // 8, 128).transpose(2, 1, 0, 3).reshape(u, d)


def _root(wide):
    return lax.rsqrt(jnp.mean(wide * wide, -1, keepdims=True) + 1e-6)


def _norm(h):
    wide = h.astype(F32)
    return (wide * _root(wide)).astype(BF)


def _norm_back(h, d):
    wide = h.astype(F32)
    scale = _root(wide)
    return scale * (d - wide * (jnp.mean(d * wide, -1, keepdims=True) * scale * scale))


def _turn(t, c, s):
    return t * c + pltpu.roll(t, HEAD // 2, 1) * s


def _turn_back(t, c, s):
    return t * c + pltpu.roll(t * s, HEAD // 2, 1)


def _heads(ref, rows):
    return jnp.concatenate([ref[i, rows, :] for i in range(ref.shape[0])], axis=1)


def _sigmoid(x):
    return 0.5 * jnp.tanh(0.5 * x) + 0.5


def _down_read(p, d):
    p = p.astype(F32)
    tall, u = d // 16, p.shape[1] // 16
    return jnp.concatenate(
        [jnp.concatenate([p[at + 8 * t : at + 8 * t + 8, 128 * s : 128 * s + 128] for t in range(d // 128)], axis=1)
         for at in range(0, p.shape[0], tall) for s in range(u // 8)], axis=0).astype(BF)


def _down_write(w, u):
    d = w.shape[1]
    return jnp.concatenate(
        [jnp.concatenate([w[at + 8 * s : at + 8 * s + 8, 128 * t : 128 * t + 128] for s in range(u // 8)], axis=1)
         for at in range(0, w.shape[0], u) for t in range(d // 128)], axis=0).astype(BF)


def _qkv(h_ref, wkv_ref, wq_ref, c_ref, s_ref, q_ref, k_ref, v_ref):
    a = _norm(h_ref[...])
    c, s = c_ref[...], s_ref[...]
    kv = _dot(a, wkv_ref[...], 1, 0).astype(BF)
    k_ref[...] = _turn(kv[:, :HEAD].astype(F32), c, s).astype(BF)
    v_ref[...] = kv[:, HEAD:]
    q = _dot(a, wq_ref[...], 1, 0).astype(BF)
    for i in range(q_ref.shape[0]):
        q_ref[i] = _turn(q[:, i * HEAD : (i + 1) * HEAD].astype(F32), c, s).astype(BF)


def _mlp(h_ref, o_ref, wo_ref, wg_ref, wu_ref, wd_ref, mid_ref, y_ref, b_s, sum_s, wd_s):
    j = pl.program_id(0)
    tokens, d = h_ref.shape

    @pl.when(j == 0)
    def _():
        def piece(n, _):
            rows = pl.ds(pl.multiple_of(n * ROWS, ROWS), ROWS)
            mid = h_ref[rows, :] + _dot(_heads(o_ref, rows), wo_ref[...], 1, 0).astype(BF)
            mid_ref[rows, :] = mid
            b_s[rows, :] = _norm(mid)
            sum_s[rows, :] = jnp.zeros((ROWS, d), F32)

        lax.fori_loop(0, tokens // ROWS, piece, None)

    wd_s[...] = _down_read(wd_ref[...], d)

    def piece(n, _):
        rows = pl.ds(pl.multiple_of(n * ROWS, ROWS), ROWS)
        gate = _dot(b_s[rows, :], wg_ref[...], 1, 0)
        up = _dot(b_s[rows, :], wu_ref[...], 1, 0)
        sum_s[rows, :] += _dot((gate * _sigmoid(gate) * up).astype(BF), wd_s[...], 1, 0)

    lax.fori_loop(0, tokens // ROWS, piece, None)

    @pl.when(j == pl.num_programs(0) - 1)
    def _():
        y_ref[...] = mid_ref[...] + sum_s[...].astype(BF)


def _mlp_back(*refs, aliased):
    if aliased:
        refs = refs[:8] + refs[9:]
    (mid_ref, dy_ref, o_ref, wo_ref, wg_ref, wu_ref, wd_ref, one_ref, dmid_ref, do_ref, delta_ref, out_ref,
     b_s, sum_s, dg_s, du_s, act_s, wd_s, pg_s, pu_s, pd_s, sem) = refs
    j, steps = pl.program_id(0), pl.num_programs(0)
    tokens, d = mid_ref.shape
    u = wd_ref.shape[1] // 16
    ff = steps * TILE
    tall = pd_s.shape[0]

    @pl.when(j == 0)
    def _():
        b_s[...] = _norm(mid_ref[...])
        sum_s[...] = jnp.zeros_like(sum_s)

    wd_s[...] = _down_read(wd_ref[...], d)

    def piece(n, _):
        rows = pl.ds(pl.multiple_of(n * ROWS, ROWS), ROWS)
        gate = _dot(b_s[rows, :], wg_ref[...], 1, 0)
        up = _dot(b_s[rows, :], wu_ref[...], 1, 0)
        dact = _dot(dy_ref[rows, :], wd_s[...], 1, 1).astype(BF).astype(F32)
        sig = _sigmoid(gate)
        silu = gate * sig
        act_s[rows, :] = (silu * up).astype(BF)
        du = (dact * silu).astype(BF)
        dg = (dact * up * (sig + silu * (1.0 - sig))).astype(BF)
        du_s[rows, :] = du
        dg_s[rows, :] = dg
        sum_s[rows, :] += _dot(dg, wg_ref[...], 1, 1) + _dot(du, wu_ref[...], 1, 1)

    lax.fori_loop(0, tokens // ROWS, piece, None)

    def copies(at):
        return (pltpu.make_async_copy(pg_s, out_ref.at[:, pl.ds(pl.multiple_of(at * TILE, TILE), TILE)], sem.at[0]),
                pltpu.make_async_copy(pu_s, out_ref.at[:, pl.ds(pl.multiple_of(ff + at * TILE, TILE), TILE)], sem.at[1]),
                pltpu.make_async_copy(pd_s, out_ref.at[pl.ds(pl.multiple_of(at * tall, tall), tall), pl.ds(2 * ff, 16 * u)], sem.at[2]))

    @pl.when(j > 0)
    def _():
        for one in copies(j - 1):
            one.wait()

    pd_s[...] = _down_write(_dot(act_s[...], dy_ref[...], 0, 0), u)
    pg_s[...] = _dot(b_s[...], dg_s[...], 0, 0).astype(BF)
    pu_s[...] = _dot(b_s[...], du_s[...], 0, 0).astype(BF)
    for one in copies(j):
        one.start()

    @pl.when(j == steps - 1)
    def _():
        def piece(n, _):
            rows = pl.ds(pl.multiple_of(n * ROWS, ROWS), ROWS)
            back = _norm_back(mid_ref[rows, :], sum_s[rows, :].astype(BF).astype(F32))
            dmid = dy_ref[rows, :] + back.astype(BF)
            dmid_ref[rows, :] = dmid
            do = _dot(dmid, wo_ref[...], 1, 1).astype(BF)
            for i in range(do_ref.shape[0]):
                mine = do[:, i * HEAD : (i + 1) * HEAD]
                do_ref[i, rows, :] = mine
                both = mine.astype(F32) * o_ref[i, rows, :].astype(F32)
                total = lax.dot_general(one_ref[...], both, (((1,), (1,)), ((), ())), precision=lax.Precision.HIGHEST,
                                        preferred_element_type=F32)
                delta_ref[i : i + 1, rows] = total[0:1, :]

        lax.fori_loop(0, tokens // ROWS, piece, None)
        for one in copies(j):
            one.wait()


def _qkv_back(*refs, at, deeper):
    dq_ref, dk_ref, dv_ref, c_ref, s_ref, h_ref, dmid_ref, o_ref, wkv_ref, wq_ref = refs[:10]
    refs = refs[10:]
    dh_ref, refs = (refs[0], refs[1:]) if deeper else (None, refs)
    out_ref, a_s, dq_s, dkv_s, p_s, sem = refs
    tokens, d = h_ref.shape

    def piece(n, _):
        rows = pl.ds(pl.multiple_of(n * ROWS, ROWS), ROWS)
        c, s = c_ref[rows, :], s_ref[rows, :]
        a_s[rows, :] = _norm(h_ref[rows, :])
        dkv_s[rows, :HEAD] = _turn_back(dk_ref[rows, :].astype(F32), c, s).astype(BF)
        dkv_s[rows, HEAD:] = dv_ref[rows, :]
        for i in range(dq_ref.shape[0]):
            dq_s[rows, i * HEAD : (i + 1) * HEAD] = _turn_back(dq_ref[i, rows, :].astype(F32), c, s).astype(BF)
        if deeper:
            da = _dot(dkv_s[rows, :], wkv_ref[...], 1, 1) + _dot(dq_s[rows, :], wq_ref[...], 1, 1)
            dh_ref[rows, :] = dmid_ref[rows, :] + _norm_back(h_ref[rows, :], da.astype(BF).astype(F32)).astype(BF)

    lax.fori_loop(0, tokens // ROWS, piece, None)
    for i in range(o_ref.shape[0]):
        p_s[i * HEAD : (i + 1) * HEAD, :d] = _dot(o_ref[i], dmid_ref[...], 0, 0).astype(BF)
    dq = dq_s.shape[1]
    p_s[:, d : d + dq] = _dot(a_s[...], dq_s[...], 0, 0).astype(BF)
    p_s[:, d + dq :] = _dot(a_s[...], dkv_s[...], 0, 0).astype(BF)
    copy = pltpu.make_async_copy(p_s, out_ref.at[:, pl.ds(at, p_s.shape[1])], sem)
    copy.start()
    copy.wait()


def _greet(others):
    barrier = pltpu.get_barrier_semaphore()
    for other in others:
        pl.semaphore_signal(barrier, inc=1, device_id={"dp": other}, device_id_type=MESH)
    pl.semaphore_wait(barrier, len(others))


def _send(src, dst, sems, at, other):
    return pltpu.make_async_remote_copy(src_ref=src, dst_ref=dst, send_sem=sems.at[0, at], recv_sem=sems.at[1, at],
                                        device_id={"dp": other}, device_id_type=MESH)


def _gather(*refs, n, layers):
    mine, out, (own_sem, ring_sems, core_sems) = refs[:layers], refs[layers : 2 * layers], refs[2 * layers :]
    me = lax.axis_index("dp")
    rows = mine[0].shape[0]
    chips = n // 2
    partner = me + 1 - 2 * lax.rem(me, 2)
    right, left = lax.rem(me + 2, n), lax.rem(me + n - 2, n)

    def block(i, owner):
        return out[i].at[pl.ds(pl.multiple_of(owner * rows, 8), rows), :]

    def owner_at(way, distance):
        return lax.rem(me + (n - 2 * distance if way == 0 else 2 * distance), n)

    _greet((right, left, partner))
    own = [pltpu.make_async_copy(mine[i], block(i, me), own_sem.at[i]) for i in range(layers)]
    for one in own:
        one.start()
    half = chips // 2
    reach = lambda way, i: half if way == i % 2 else chips - 1 - half
    ring, core = {}, {}
    for distance in range(half + 1):
        for i in range(layers):
            for way in range(2):
                if distance > reach(way, i):
                    continue
                owner = owner_at(way, distance)
                if distance:
                    ring[way, i, distance - 1].wait_recv()
                src = block(i, owner) if distance else mine[i]
                if distance < reach(way, i):
                    at = (way * layers + i) * half + distance
                    ring[way, i, distance] = _send(src, block(i, owner), ring_sems, at, (right, left)[way])
                    ring[way, i, distance].start()
                if distance or way == 0:
                    at = (way * layers + i) * (half + 1) + distance
                    core[way, i, distance] = _send(src, block(i, owner), core_sems, at, partner)
                    core[way, i, distance].start()
    for one in (*ring.values(), *core.values()):
        one.wait_send()
    for one in core.values():
        one.wait_recv()
    for one in own:
        one.wait()


def gathered(blocks, n):
    layers, (rows, columns) = len(blocks), blocks[0].shape
    half = n // 4
    return pl.pallas_call(
        functools.partial(_gather, n=n, layers=layers), name="gather", out_shape=[_like(n * rows, columns)] * layers,
        in_specs=[pl.BlockSpec(memory_space=pltpu.VMEM)] * layers, out_specs=[pl.BlockSpec(memory_space=pl.ANY)] * layers,
        scratch_shapes=[pltpu.SemaphoreType.DMA((layers,)), pltpu.SemaphoreType.DMA((2, 2 * layers * half)),
                        pltpu.SemaphoreType.DMA((2, 2 * layers * (half + 1)))],
        compiler_params=pltpu.CompilerParams(collective_id=0, has_side_effects=True))(*blocks)


def _scatter(x_ref, out_ref, mine, theirs, both, far, sem, core_sems, ring_sems, *, n):
    me = lax.axis_index("dp")
    rows = out_ref.shape[0]
    chips = n // 2
    core = lax.rem(me, 2)
    chip = lax.div(me, 2)
    partner = me + 1 - 2 * core
    away = [lax.rem(chip + k, chips) for k in range(chips)]
    _greet((partner, *(2 * away[k] + core for k in range(1, chips))))

    def block(owner):
        return x_ref.at[pl.ds(pl.multiple_of(owner * rows, 8), rows), :]

    over = [_send(block(2 * away[k] + 1 - core), theirs.at[k], core_sems, k, partner) for k in range(chips)]
    own = [pltpu.make_async_copy(block(2 * away[k] + core), mine.at[k], sem.at[k]) for k in range(chips)]
    for one in (*over, *own):
        one.start()
    for one in own:
        one.wait()
    for one in over:
        one.wait()
    for k in range(1, chips):
        both[k] = (mine[k].astype(F32) + theirs[k].astype(F32)).astype(BF)
    out = [_send(both.at[k], far.at[k], ring_sems, k, 2 * away[k] + core) for k in range(1, chips)]
    for one in out:
        one.start()
    total = mine[0].astype(F32) + theirs[0].astype(F32)
    for one in out:
        one.wait()
    for k in range(1, chips):
        total = total + far[k].astype(F32)
    out_ref[...] = total.astype(BF)


def scattered(x, n):
    rows, columns = x.shape[0] // n, x.shape[1]
    chips = n // 2
    slots = pltpu.VMEM((chips, rows, columns), BF)
    return pl.pallas_call(
        functools.partial(_scatter, n=n), name="scatter", out_shape=_like(rows, columns), in_specs=[pl.BlockSpec(memory_space=pl.ANY)],
        out_specs=pl.BlockSpec(memory_space=pltpu.VMEM),
        scratch_shapes=[slots] * 4 + [pltpu.SemaphoreType.DMA((chips,))] + [pltpu.SemaphoreType.DMA((2, chips))] * 2,
        compiler_params=pltpu.CompilerParams(collective_id=1, has_side_effects=True))(x)


def _clip(*refs, n):
    *piece, out_ref, tile, held, sems = refs
    me = lax.axis_index("dp")
    others = [lax.rem(me + k, n) for k in range(1, n)]
    _greet(others)
    squares, count = jnp.zeros((1, 1), F32), 0
    for p in piece:
        count += n * p.shape[0] * p.shape[1]
        squares = squares + jnp.sum(jnp.square(p[...].astype(F32)), keepdims=True)
    tile[...] = jnp.broadcast_to(squares, tile.shape)
    out = [_send(tile, held.at[k], sems, k, other) for k, other in enumerate(others)]
    for one in out:
        one.start()
    for one in out:
        one.wait()
    total = tile[...]
    for k in range(n - 1):
        total = total + held[k]
    out_ref[...] = jnp.minimum(1.0, 0.5 * lax.rsqrt(total / count + 1e-30))


def _adamw(factor_ref, *refs, places, pieces):
    names, per = len(NAMES), 3 * len(NAMES)
    piece, given, made, bufs = (refs[a : a + c] for a, c in ((0, pieces), (pieces, per), (pieces + per, per), (pieces + 2 * per, per)))
    in_sem, out_sem = refs[pieces + 3 * per :]
    load = [pltpu.make_async_copy(a, b, in_sem.at[i]) for i, (a, b) in enumerate(zip(given, bufs))]
    for at in range(names):
        for one in load[at::names]:
            one.start()
    factor = factor_ref[0:1, 0:1]
    stored = []
    for at, name in enumerate(NAMES):
        w_ref, m_ref, v_ref = trio = bufs[at::names]
        for one in load[at::names]:
            one.wait()
        for i in range(w_ref.shape[0]):
            which, first = places[name][i]
            if name == "w_down":
                g = _down_read(piece[which][:, first : first + 16 * w_ref.shape[1]], w_ref.shape[2])
            else:
                g = piece[which][:, first : first + w_ref.shape[2]]
            g = g.astype(F32) * factor
            m = 0.9 * m_ref[i] + 0.1 * g
            v = 0.95 * v_ref[i] + 0.05 * g * g
            w = w_ref[i].astype(F32)
            w_ref[i] = (w - 0.02 * (m * lax.rsqrt(v + 1e-8) + 0.1 * w)).astype(BF)
            m_ref[i] = m
            v_ref[i] = v
        for a, b, k in zip(trio, made[at::names], range(at, per, names)):
            stored.append(pltpu.make_async_copy(a, b, out_sem.at[k]))
            stored[-1].start()
    for one in stored:
        one.wait()


def finished(pieces, arrays, places, n):
    vmem, anywhere = pl.BlockSpec(memory_space=pltpu.VMEM), pl.BlockSpec(memory_space=pl.ANY)
    small = pltpu.VMEM((8, HEAD), F32)
    count = len(arrays)
    factor = pl.pallas_call(
        functools.partial(_clip, n=n), name="clip", out_shape=_like(8, HEAD, dtype=F32), in_specs=[vmem] * len(pieces), out_specs=vmem,
        scratch_shapes=[small, pltpu.VMEM((n - 1, 8, HEAD), F32), pltpu.SemaphoreType.DMA((2, n - 1))],
        compiler_params=pltpu.CompilerParams(collective_id=2, has_side_effects=True))(*pieces)
    return pl.pallas_call(
        functools.partial(_adamw, places=places, pieces=len(pieces)), name="adamw", out_shape=[_like(*a.shape, dtype=a.dtype) for a in arrays],
        in_specs=[vmem] * (1 + len(pieces)) + [anywhere] * count, out_specs=[anywhere] * count,
        scratch_shapes=[pltpu.VMEM(a.shape, a.dtype) for a in arrays] + [pltpu.SemaphoreType.DMA((count,))] * 2,
        compiler_params=pltpu.CompilerParams(vmem_limit_bytes=VMEM))(factor, *pieces, *arrays)


def _price(flops, *arrays):
    return pl.CostEstimate(flops=int(flops), transcendentals=0, bytes_accessed=int(sum(a.size * a.dtype.itemsize for a in arrays)))


def _whole(shape):
    return pl.BlockSpec(shape, lambda *_: (0,) * len(shape))


def _like(*shape, dtype=BF):
    return jax.ShapeDtypeStruct(shape, dtype)


def solution(mesh):
    n = mesh.shape["dp"]

    def step(x, dy, *arrays):
        weights = dict(zip(NAMES, arrays[: len(NAMES)], strict=True))
        layers, ff, d = weights["wq"].shape[0], weights["w_gate"].shape[2], x.shape[2]
        tokens = x.shape[1]
        dq, kv = weights["wq"].shape[2], 2 * weights["wk"].shape[2]
        heads, u = dq // HEAD, ff // n
        mlp, att = 3 * ff, kv + d + dq
        tall = TILE // u * (d // 16)
        keep = _params()
        anywhere = pl.BlockSpec(memory_space=pl.ANY)

        angle = jnp.arange(tokens, dtype=F32)[:, None] * THETA ** (-jnp.arange(HEAD // 2, dtype=F32) / (HEAD // 2))
        cos, sin = jnp.cos(angle), jnp.sin(angle)
        c, s = jnp.concatenate([cos, cos], 1), jnp.concatenate([-sin, sin], 1)

        beside = lambda names, i: jnp.concatenate([weights[name][i] for name in names], 1)
        around = gathered([beside(("wo", "wq", "wk", "wv"), i) for i in range(layers)], n)
        middle = [lax.all_gather(jnp.concatenate([beside(("w_gate", "w_up"), i), packed_down(weights["w_down"][i])], 1), "dp", axis=0, tiled=True)
                  for i in range(layers)]

        w_o, w_q, w_kv = (pl.BlockSpec((d, width), lambda *_, at=start // width: (0, at)) for width, start in ((d, 0), (dq, d), (kv, d + dq)))
        w_gate = pl.BlockSpec((d, TILE), lambda j: (0, j))
        w_up = pl.BlockSpec((d, TILE), lambda j: (0, ff // TILE + j))
        w_down = pl.BlockSpec((tall, ff), lambda j: (j, 2))

        def qkv(h, w):
            rows = 256
            block = lambda width: pl.BlockSpec((rows, width), lambda j: (j, 0))
            return pl.pallas_call(
                _qkv, name="qkv", grid=(tokens // rows,), in_specs=[block(d), w_kv, w_q, block(HEAD), block(HEAD)],
                out_specs=[pl.BlockSpec((heads, rows, HEAD), lambda j: (0, j, 0)), block(HEAD), block(HEAD)],
                out_shape=[_like(heads, tokens, HEAD), _like(tokens, HEAD), _like(tokens, HEAD)], compiler_params=keep,
                cost_estimate=_price(2 * tokens * d * (dq + kv), h, h, h))(h, w, w, c, s)

        def through_mlp(h, o, a, w):
            return pl.pallas_call(
                _mlp, name="mlp", grid=(ff // TILE,),
                in_specs=[_whole(h.shape), _whole(o.shape), w_o, w_gate, w_up, w_down],
                out_specs=[_whole(h.shape), _whole(h.shape)], out_shape=[_like(*h.shape), _like(*h.shape)],
                scratch_shapes=[pltpu.VMEM(h.shape, BF), pltpu.VMEM(h.shape, F32), pltpu.VMEM((TILE, d), BF)], compiler_params=keep,
                cost_estimate=_price(2 * tokens * d * (mlp + d), h, h, h, w))(h, o, a, w, w, w)

        def mlp_back(mid, dh, o, a, w, into):
            given = [mid, dh, o, a, w, w, w, jnp.ones((8, HEAD), F32)]
            specs = [_whole(mid.shape), _whole(mid.shape), _whole(o.shape), w_o, w_gate, w_up, w_down, _whole((8, HEAD))]
            out = _like(d, mlp) if into is None else into
            wide = pltpu.VMEM((tokens, TILE), BF)
            return pl.pallas_call(
                functools.partial(_mlp_back, aliased=into is not None), name="mlp_back", grid=(ff // TILE,),
                in_specs=specs + ([] if into is None else [anywhere]),
                out_specs=[_whole(mid.shape), _whole(o.shape), _whole((heads, tokens)), anywhere],
                out_shape=[_like(*mid.shape), _like(*o.shape), _like(heads, tokens, dtype=F32), _like(*out.shape)],
                input_output_aliases={} if into is None else {8: 3},
                scratch_shapes=[pltpu.VMEM(mid.shape, BF), pltpu.VMEM(mid.shape, F32), wide, wide, wide, pltpu.VMEM((TILE, d), BF),
                                pltpu.VMEM((d, TILE), BF), pltpu.VMEM((d, TILE), BF), pltpu.VMEM((tall, ff), BF),
                                pltpu.SemaphoreType.DMA((3,))],
                compiler_params=keep, cost_estimate=_price(2 * tokens * d * (8 * ff + d), mid, mid, mid, w, w),
            )(*given, *([] if into is None else [into]))

        def qkv_back(parts, h, dmid, o, w, at, columns, deeper):
            given = [*parts, c, s, h, dmid, o, w, w]
            specs = [_whole(a.shape) for a in given[:-2]] + [w_kv, w_q]
            out = _like(d, columns)
            got = pl.pallas_call(
                functools.partial(_qkv_back, at=at, deeper=deeper), name="qkv_back", grid=(1,),
                in_specs=specs, out_specs=([_whole(h.shape)] if deeper else []) + [anywhere],
                out_shape=([_like(*h.shape)] if deeper else []) + [out],
                scratch_shapes=[pltpu.VMEM(h.shape, BF), pltpu.VMEM((tokens, dq), BF), pltpu.VMEM((tokens, kv), BF),
                                pltpu.VMEM((d, att), BF), pltpu.SemaphoreType.DMA],
                compiler_params=keep, cost_estimate=_price(4 * tokens * d * att, h, h, h, h, h))(*given)
            return got if deeper else [None, got[0]]

        h, kept = x[0], []
        for i in range(layers):
            q, k, v = qkv(h, around[i])
            o, lse = attend(q, k, v)
            mid, after = through_mlp(h, o, around[i], middle[i])
            kept.append((h, q, k, v, o, lse, mid))
            h = after

        dh, into, pieces = dy[0], None, [None] * layers
        for i in reversed(range(layers)):
            h, q, k, v, o, lse, mid = kept[i]
            dmid, do, delta, into = mlp_back(mid, dh, o, around[i], middle[i], into)
            pieces[i] = lax.psum_scatter(into, "dp", scatter_dimension=0, tiled=True)
            parts = attend_bwd(q, k, v, do, lse, delta)
            dh, into = qkv_back(parts, h, dmid, o, around[i], mlp if i else 0, mlp + att if i else att, i > 0)
        pieces.append(scattered(into, n))

        places = {name: [(i, at) for i in range(layers)] for name, at in (("w_gate", 0), ("w_up", ff), ("w_down", 2 * ff))}
        for name, at in (("wo", 0), ("wq", d), ("wk", d + dq), ("wv", d + dq + kv // 2)):
            places[name] = [(i - 1, mlp + at) if i else (layers, at) for i in range(layers)]
        return tuple(finished(pieces, arrays, places, n))

    states, cut = P(("rep", "dp"), None, None), P(None, "dp", None)
    return jax.shard_map(
        step,
        mesh=mesh,
        in_specs=(states, states) + (cut,) * 21,
        out_specs=(P("rep", "dp", None),) * 21,
        check_vma=False,
    )
```

```python
import functools

import jax
import jax.numpy as jnp
from jax import lax
from jax.experimental import pallas as pl
from jax.experimental.pallas import tpu as pltpu
from jax.sharding import PartitionSpec as P

NEG = -1e30
HIDDEN = 2 * NEG
LOG2E = 1.4426950408889634
VMEM = 56 * 2**20
STRIP = 512
BQ = 512
BQ_BACK = 256
BK = 256


def _dot(a, b, ca, cb):
    return lax.dot_general(a, b, (((ca,), (cb,)), ((), ())), preferred_element_type=jnp.float32)


def _strips(cols):
    width = max(w for w in range(HEAD, STRIP + 1, HEAD) if cols % w == 0)
    return width, range(0, cols, width)


def _gap(bk, cols, bq):
    return lax.rem(lax.broadcasted_iota(jnp.int32, (bk, cols), 1), bq) - lax.broadcasted_iota(jnp.int32, (bk, cols), 0)


def _row(ref):
    return jnp.concatenate([ref[i : i + 1, :] for i in range(ref.shape[0])], axis=1)


def _over_keys(block, iq, bq, bk):
    whole, last = lax.div(iq * bq, bk), lax.div(iq * bq + bq, bk)
    lax.fori_loop(0, whole, lambda j, _: block(j, False), None)
    lax.fori_loop(whole, last, lambda j, _: block(j, True), None)


def _forward(q_ref, k_ref, v_ref, o_ref, lse_ref, top_s, mix_s, gap_s, *, bk):
    g, bq, d = q_ref.shape
    cols, low = g * bq, k_ref.dtype
    iq = pl.program_id(0)
    scale = d**-0.5
    e = scale * LOG2E
    wide, pieces = _strips(cols)

    @pl.when(iq == 0)
    def _():
        gap_s[...] = _gap(bk, cols, bq)

    top_s[...] = jnp.full(top_s.shape, NEG, jnp.float32)
    mix_s[...] = jnp.zeros(mix_s.shape, jnp.float32)
    ones = jnp.ones((8, bk), low)

    def block(j, masked):
        here = pl.ds(pl.multiple_of(j * bk, bk), bk)
        scores = [_dot(k_ref[here, :], q_ref[...].reshape(cols, d)[at : at + wide, :], 1, 1) for at in pieces]
        weights, keeps = [], []
        for at, s in zip(pieces, scores):
            if masked:
                s = jnp.where(gap_s[:, at : at + wide] >= j * bk - iq * bq, s, HIDDEN)
            old = top_s[:, at : at + wide]
            top = jnp.maximum(old, s.max(axis=0, keepdims=True))
            top_s[:, at : at + wide] = top
            weights.append(jnp.exp2((s - top) * e).astype(low))
            keeps.append(jnp.exp2((old - top) * e))
        values = jnp.concatenate([v_ref[here, :].T, ones], axis=0)
        for at, p, keep in zip(pieces, weights, keeps):
            mix_s[:, at : at + wide] = mix_s[:, at : at + wide] * keep + _dot(values, p, 1, 0)

    _over_keys(block, iq, bq, bk)
    total = mix_s[d : d + 1, :]
    o_ref[...] = (mix_s[:d, :] * (1 / total)).T.reshape(g, bq, d).astype(o_ref.dtype)
    lse = top_s[...] * scale + jnp.log(total)
    for i in range(g):
        lse_ref[i : i + 1, :] = lse[:, i * bq : (i + 1) * bq]


def _backward(q_ref, k_ref, v_ref, do_ref, lse_ref, delta_ref, dq_ref, dk_ref, dv_ref, dq_s, dk_s, dv_s, gap_s, *, bk):
    g, bq, d = q_ref.shape
    cols, low = g * bq, q_ref.dtype
    iq = pl.program_id(0)
    scale = d**-0.5
    e = scale * LOG2E
    wide, pieces = _strips(cols)

    @pl.when(iq == 0)
    def _():
        gap_s[...] = _gap(bk, cols, bq)
        dk_s[...] = jnp.zeros_like(dk_s)
        dv_s[...] = jnp.zeros_like(dv_s)

    dq_s[...] = jnp.zeros_like(dq_s)
    lses, deltas = _row(lse_ref) * LOG2E, _row(delta_ref)

    def block(j, masked):
        here = pl.ds(pl.multiple_of(j * bk, bk), bk)
        qs = [q_ref[...].reshape(cols, d)[at : at + wide, :] for at in pieces]
        dos = [do_ref[...].reshape(cols, d)[at : at + wide, :] for at in pieces]
        scores = [_dot(k_ref[here, :], one, 1, 1) for one in qs]
        dps = [_dot(v_ref[here, :], one, 1, 1) for one in dos]
        for at, q, do, s, dp in zip(pieces, qs, dos, scores, dps):
            p = jnp.exp2(s * e - lses[:, at : at + wide])
            if masked:
                p = jnp.where(gap_s[:, at : at + wide] >= j * bk - iq * bq, p, 0.0)
            ds = (p * (dp - deltas[:, at : at + wide])).astype(low)
            dv_s[here, :] += _dot(p.astype(low), do, 1, 0)
            dk_s[here, :] += _dot(ds, q, 1, 0)
            dq_s[:, at : at + wide] += _dot(k_ref[here, :].T, ds, 1, 0)

    _over_keys(block, iq, bq, bk)
    dq_ref[...] = (dq_s[...] * scale).T.reshape(g, bq, d).astype(dq_ref.dtype)

    @pl.when(iq == pl.num_programs(0) - 1)
    def _():
        dk_ref[...] = (dk_s[...] * scale).astype(dk_ref.dtype)
        dv_ref[...] = dv_s[...].astype(dv_ref.dtype)


def _specs(q, bq):
    g, tokens, d = q.shape
    return (pl.BlockSpec((g, bq, d), lambda iq: (0, iq, 0)), pl.BlockSpec((tokens, d), lambda iq: (0, 0)),
            pl.BlockSpec((g, bq), lambda iq: (0, iq)))


def _params():
    return pltpu.CompilerParams(vmem_limit_bytes=VMEM, dimension_semantics=("arbitrary",))


def attend(q, k, v):
    g, tokens, d = q.shape
    queries, keys, stats = _specs(q, BQ)
    bk, cols = BK, g * BQ
    return pl.pallas_call(
        functools.partial(_forward, bk=bk), name="attend", grid=(tokens // BQ,), in_specs=[queries, keys, keys], out_specs=[queries, stats],
        out_shape=[_like(*q.shape), _like(g, tokens, dtype=F32)],
        scratch_shapes=[pltpu.VMEM((1, cols), F32), pltpu.VMEM((d + 8, cols), F32), pltpu.VMEM((bk, cols), jnp.int32)],
        compiler_params=_params(), cost_estimate=_price(4 * g * tokens * tokens * d, q, q, k, v))(q, k, v)


def attend_bwd(q, k, v, do, lse, delta):
    g, tokens, d = q.shape
    queries, keys, stats = _specs(q, BQ_BACK)
    bk, cols = BK, g * BQ_BACK
    return pl.pallas_call(
        functools.partial(_backward, bk=bk), name="attend_back", grid=(tokens // BQ_BACK,),
        in_specs=[queries, keys, keys, queries, stats, stats], out_specs=[queries, keys, keys],
        out_shape=[_like(*q.shape), _like(*k.shape), _like(*v.shape)],
        scratch_shapes=[pltpu.VMEM((d, cols), F32), pltpu.VMEM((tokens, d), F32), pltpu.VMEM((tokens, d), F32),
                        pltpu.VMEM((bk, cols), jnp.int32)],
        compiler_params=_params(), cost_estimate=_price(10 * g * tokens * tokens * d, q, q, q, k, v))(q, k, v, do, lse, delta)


HEAD = 128
THETA = 10000
NAMES = ("wq", "wk", "wv", "wo", "w_gate", "w_up", "w_down")
BF, F32 = jnp.bfloat16, jnp.float32
TILE = 512
ROWS = 256
MESH = pl.DeviceIdType.MESH


def packed_down(w):
    u, d = w.shape
    return w.reshape(u // 8, 8, d // 128, 128).transpose(2, 1, 0, 3).reshape(d // 16, 16 * u)


def unpacked_down(p):
    d, u = p.shape[0] * 16, p.shape[1] // 16
    return p.reshape(d // 128, 8, u // 8, 128).transpose(2, 1, 0, 3).reshape(u, d)


def _root(wide):
    return lax.rsqrt(jnp.mean(wide * wide, -1, keepdims=True) + 1e-6)


def _norm(h):
    wide = h.astype(F32)
    return (wide * _root(wide)).astype(BF)


def _norm_back(h, d):
    wide = h.astype(F32)
    scale = _root(wide)
    return scale * (d - wide * (jnp.mean(d * wide, -1, keepdims=True) * scale * scale))


def _turn(t, c, s):
    return t * c + pltpu.roll(t, HEAD // 2, 1) * s


def _turn_back(t, c, s):
    return t * c + pltpu.roll(t * s, HEAD // 2, 1)


def _heads(ref, rows):
    return jnp.concatenate([ref[i, rows, :] for i in range(ref.shape[0])], axis=1)


def _sigmoid(x):
    return 0.5 * jnp.tanh(0.5 * x) + 0.5


def _down_read(p, d):
    p = p.astype(F32)
    tall, u = d // 16, p.shape[1] // 16
    return jnp.concatenate(
        [jnp.concatenate([p[at + 8 * t : at + 8 * t + 8, 128 * s : 128 * s + 128] for t in range(d // 128)], axis=1)
         for at in range(0, p.shape[0], tall) for s in range(u // 8)], axis=0).astype(BF)


def _down_write(w, u):
    d = w.shape[1]
    return jnp.concatenate(
        [jnp.concatenate([w[at + 8 * s : at + 8 * s + 8, 128 * t : 128 * t + 128] for s in range(u // 8)], axis=1)
         for at in range(0, w.shape[0], u) for t in range(d // 128)], axis=0).astype(BF)


def _staggered(front, middle, count):
    held = front(0)
    for n in range(count):
        later = front(n + 1) if n + 1 < count else None
        middle(n, *held)
        held = later


def _qkv(h_ref, wkv_ref, wq_ref, c_ref, s_ref, q_ref, k_ref, v_ref):
    a = _norm(h_ref[...])
    c, s = c_ref[...], s_ref[...]
    kv = _dot(a, wkv_ref[...], 1, 0).astype(BF)
    k_ref[...] = _turn(kv[:, :HEAD].astype(F32), c, s).astype(BF)
    v_ref[...] = kv[:, HEAD:]
    q = _dot(a, wq_ref[...], 1, 0).astype(BF)
    for i in range(q_ref.shape[0]):
        q_ref[i] = _turn(q[:, i * HEAD : (i + 1) * HEAD].astype(F32), c, s).astype(BF)


def _mlp(h_ref, o_ref, wo_ref, wg_ref, wu_ref, wd_ref, mid_ref, y_ref, b_s, sum_s, act_s, wd_s):
    j = pl.program_id(0)
    tokens, d = h_ref.shape

    @pl.when(j == 0)
    def _():
        def piece(n, _):
            rows = pl.ds(pl.multiple_of(n * ROWS, ROWS), ROWS)
            mid = h_ref[rows, :] + _dot(_heads(o_ref, rows), wo_ref[...], 1, 0).astype(BF)
            mid_ref[rows, :] = mid
            b_s[rows, :] = _norm(mid)
            sum_s[rows, :] = jnp.zeros((ROWS, d), F32)

        lax.fori_loop(0, tokens // ROWS, piece, None)

    wd_s[...] = _down_read(wd_ref[...], d)

    def front(n):
        rows = pl.ds(n * ROWS, ROWS)
        return _dot(b_s[rows, :], wg_ref[...], 1, 0), _dot(b_s[rows, :], wu_ref[...], 1, 0)

    def middle(n, gate, up):
        act_s[pl.ds(n * ROWS, ROWS), :] = (gate * _sigmoid(gate) * up).astype(BF)

    _staggered(front, middle, tokens // ROWS)
    sum_s[...] += _dot(act_s[...], wd_s[...], 1, 0)

    @pl.when(j == pl.num_programs(0) - 1)
    def _():
        y_ref[...] = mid_ref[...] + sum_s[...].astype(BF)


def _mlp_back(*refs, aliased):
    if aliased:
        refs = refs[:8] + refs[9:]
    (mid_ref, dy_ref, o_ref, wo_ref, wg_ref, wu_ref, wd_ref, one_ref, dmid_ref, do_ref, delta_ref, out_ref,
     b_s, sum_s, dg_s, du_s, act_s, wd_s, pg_s, pu_s, pd_s, sem) = refs
    j, steps = pl.program_id(0), pl.num_programs(0)
    tokens, d = mid_ref.shape
    u = wd_ref.shape[1] // 16
    ff = steps * TILE
    tall = pd_s.shape[0]

    @pl.when(j == 0)
    def _():
        b_s[...] = _norm(mid_ref[...])
        sum_s[...] = jnp.zeros_like(sum_s)

    wd_s[...] = _down_read(wd_ref[...], d)

    def front(n):
        rows = pl.ds(n * ROWS, ROWS)
        gate = _dot(b_s[rows, :], wg_ref[...], 1, 0)
        up = _dot(b_s[rows, :], wu_ref[...], 1, 0)
        return gate, up, _dot(dy_ref[rows, :], wd_s[...], 1, 1)

    def middle(n, gate, up, dact):
        rows = pl.ds(n * ROWS, ROWS)
        dact = dact.astype(BF).astype(F32)
        sig = _sigmoid(gate)
        silu = gate * sig
        act_s[rows, :] = (silu * up).astype(BF)
        du_s[rows, :] = (dact * silu).astype(BF)
        dg_s[rows, :] = (dact * up * (sig + silu * (1.0 - sig))).astype(BF)

    _staggered(front, middle, tokens // ROWS)
    sum_s[...] += _dot(dg_s[...], wg_ref[...], 1, 1) + _dot(du_s[...], wu_ref[...], 1, 1)

    def copies(at):
        return (pltpu.make_async_copy(pg_s, out_ref.at[:, pl.ds(pl.multiple_of(at * TILE, TILE), TILE)], sem.at[0]),
                pltpu.make_async_copy(pu_s, out_ref.at[:, pl.ds(pl.multiple_of(ff + at * TILE, TILE), TILE)], sem.at[1]),
                pltpu.make_async_copy(pd_s, out_ref.at[pl.ds(pl.multiple_of(at * tall, tall), tall), pl.ds(2 * ff, 16 * u)], sem.at[2]))

    @pl.when(j > 0)
    def _():
        for one in copies(j - 1):
            one.wait()

    pd_s[...] = _down_write(_dot(act_s[...], dy_ref[...], 0, 0), u)
    pg_s[...] = _dot(b_s[...], dg_s[...], 0, 0).astype(BF)
    pu_s[...] = _dot(b_s[...], du_s[...], 0, 0).astype(BF)
    for one in copies(j):
        one.start()

    @pl.when(j == steps - 1)
    def _():
        def piece(n, _):
            rows = pl.ds(pl.multiple_of(n * ROWS, ROWS), ROWS)
            back = _norm_back(mid_ref[rows, :], sum_s[rows, :].astype(BF).astype(F32))
            dmid = dy_ref[rows, :] + back.astype(BF)
            dmid_ref[rows, :] = dmid
            do = _dot(dmid, wo_ref[...], 1, 1).astype(BF)
            for i in range(do_ref.shape[0]):
                mine = do[:, i * HEAD : (i + 1) * HEAD]
                do_ref[i, rows, :] = mine
                both = mine.astype(F32) * o_ref[i, rows, :].astype(F32)
                total = lax.dot_general(one_ref[...], both, (((1,), (1,)), ((), ())), precision=lax.Precision.HIGHEST,
                                        preferred_element_type=F32)
                delta_ref[i : i + 1, rows] = total[0:1, :]

        lax.fori_loop(0, tokens // ROWS, piece, None)
        for one in copies(j):
            one.wait()


def _qkv_back(*refs, at, deeper):
    dq_ref, dk_ref, dv_ref, c_ref, s_ref, h_ref, dmid_ref, o_ref, wkv_ref, wq_ref = refs[:10]
    refs = refs[10:]
    dh_ref, refs = (refs[0], refs[1:]) if deeper else (None, refs)
    out_ref, a_s, dq_s, dkv_s, p_s, sem = refs
    tokens, d = h_ref.shape

    def piece(n, _):
        rows = pl.ds(pl.multiple_of(n * ROWS, ROWS), ROWS)
        c, s = c_ref[rows, :], s_ref[rows, :]
        a_s[rows, :] = _norm(h_ref[rows, :])
        dkv_s[rows, :HEAD] = _turn_back(dk_ref[rows, :].astype(F32), c, s).astype(BF)
        dkv_s[rows, HEAD:] = dv_ref[rows, :]
        for i in range(dq_ref.shape[0]):
            dq_s[rows, i * HEAD : (i + 1) * HEAD] = _turn_back(dq_ref[i, rows, :].astype(F32), c, s).astype(BF)
        if deeper:
            da = _dot(dkv_s[rows, :], wkv_ref[...], 1, 1) + _dot(dq_s[rows, :], wq_ref[...], 1, 1)
            dh_ref[rows, :] = dmid_ref[rows, :] + _norm_back(h_ref[rows, :], da.astype(BF).astype(F32)).astype(BF)

    lax.fori_loop(0, tokens // ROWS, piece, None)
    for i in range(o_ref.shape[0]):
        p_s[i * HEAD : (i + 1) * HEAD, :d] = _dot(o_ref[i], dmid_ref[...], 0, 0).astype(BF)
    dq = dq_s.shape[1]
    p_s[:, d : d + dq] = _dot(a_s[...], dq_s[...], 0, 0).astype(BF)
    p_s[:, d + dq :] = _dot(a_s[...], dkv_s[...], 0, 0).astype(BF)
    copy = pltpu.make_async_copy(p_s, out_ref.at[:, pl.ds(at, p_s.shape[1])], sem)
    copy.start()
    copy.wait()


def _greet(others):
    barrier = pltpu.get_barrier_semaphore()
    for other in others:
        pl.semaphore_signal(barrier, inc=1, device_id={"dp": other}, device_id_type=MESH)
    pl.semaphore_wait(barrier, len(others))


def _send(src, dst, sems, at, other):
    return pltpu.make_async_remote_copy(src_ref=src, dst_ref=dst, send_sem=sems.at[0, at], recv_sem=sems.at[1, at],
                                        device_id={"dp": other}, device_id_type=MESH)


def _gather(*refs, n, layers):
    mine, out, (own_sem, ring_sems, core_sems) = refs[:layers], refs[layers : 2 * layers], refs[2 * layers :]
    me = lax.axis_index("dp")
    rows = mine[0].shape[0]
    chips = n // 2
    partner = me + 1 - 2 * lax.rem(me, 2)
    right, left = lax.rem(me + 2, n), lax.rem(me + n - 2, n)

    def block(i, owner):
        return out[i].at[pl.ds(pl.multiple_of(owner * rows, 8), rows), :]

    def owner_at(way, distance):
        return lax.rem(me + (n - 2 * distance if way == 0 else 2 * distance), n)

    _greet((right, left, partner))
    own = [pltpu.make_async_copy(mine[i], block(i, me), own_sem.at[i]) for i in range(layers)]
    for one in own:
        one.start()
    half = chips // 2
    reach = lambda way, i: half if way == i % 2 else chips - 1 - half
    ring, core = {}, {}
    for distance in range(half + 1):
        for i in range(layers):
            for way in range(2):
                if distance > reach(way, i):
                    continue
                owner = owner_at(way, distance)
                if distance:
                    ring[way, i, distance - 1].wait_recv()
                src = block(i, owner) if distance else mine[i]
                if distance < reach(way, i):
                    at = (way * layers + i) * half + distance
                    ring[way, i, distance] = _send(src, block(i, owner), ring_sems, at, (right, left)[way])
                    ring[way, i, distance].start()
                if distance or way == 0:
                    at = (way * layers + i) * (half + 1) + distance
                    core[way, i, distance] = _send(src, block(i, owner), core_sems, at, partner)
                    core[way, i, distance].start()
    for one in (*ring.values(), *core.values()):
        one.wait_send()
    for one in core.values():
        one.wait_recv()
    for one in own:
        one.wait()


def gathered(blocks, n):
    layers, (rows, columns) = len(blocks), blocks[0].shape
    half = n // 4
    return pl.pallas_call(
        functools.partial(_gather, n=n, layers=layers), name="gather", out_shape=[_like(n * rows, columns)] * layers,
        in_specs=[pl.BlockSpec(memory_space=pltpu.VMEM)] * layers, out_specs=[pl.BlockSpec(memory_space=pl.ANY)] * layers,
        scratch_shapes=[pltpu.SemaphoreType.DMA((layers,)), pltpu.SemaphoreType.DMA((2, 2 * layers * half)),
                        pltpu.SemaphoreType.DMA((2, 2 * layers * (half + 1)))],
        compiler_params=pltpu.CompilerParams(collective_id=0, has_side_effects=True))(*blocks)


def _scatter(x_ref, out_ref, mine, theirs, *rest, n):
    slots, (sem, core_sems), ways_sems = (rest[0:2], rest[2:4]), rest[4:6], rest[6:8]
    me = lax.axis_index("dp")
    rows = out_ref.shape[0]
    chips = n // 2
    core, chip = lax.rem(me, 2), lax.div(me, 2)
    partner = me + 1 - 2 * core
    away = [lax.rem(chip + k, chips) for k in range(chips)]
    sides = [2 * away[k] + core for k in (1, chips - 1)]
    _greet((partner, *sides))

    def block(owner):
        return x_ref.at[pl.ds(pl.multiple_of(owner * rows, 8), rows), :]

    first = [chips // 2, chips // 2 + 1]
    steps, stride = [chips // 2, chips - 1 - chips // 2], [chips - 1, 1]
    order = [k % chips for k in range(first[0], first[0] + chips)]
    over = [_send(block(2 * away[k] + 1 - core), theirs.at[k], core_sems, k, partner) for k in order]
    own = [pltpu.make_async_copy(block(2 * away[k] + core), mine.at[k], sem.at[k]) for k in order]
    for one in (*over, *own):
        one.start()
    for one in (*own, *over):
        one.wait()
    total = lambda k: mine[k].astype(F32) + theirs[k].astype(F32)
    sent = {}
    for step in range(max(steps) + 1):
        for way in range(2):
            out, into = slots[way]
            if step > steps[way]:
                continue
            if step:
                sent[way, step - 1].wait_recv()
            if step < steps[way]:
                term = total((first[way] + step * stride[way]) % chips)
                out[step] = (term + into[step - 1].astype(F32) if step else term).astype(BF)
                sent[way, step] = _send(out.at[step], into.at[step], ways_sems[way], step, sides[way])
                sent[way, step].start()
    out_ref[...] = (total(0) + sum(slots[way][1][steps[way] - 1].astype(F32) for way in range(2))).astype(BF)
    for one in sent.values():
        one.wait_send()


def scattered(x, n):
    rows, columns = x.shape[0] // n, x.shape[1]
    chips = n // 2
    slots = lambda count: pltpu.VMEM((count, rows, columns), BF)
    far, sems = (chips // 2, chips - 1 - chips // 2), lambda count: pltpu.SemaphoreType.DMA((2, count))
    return pl.pallas_call(
        functools.partial(_scatter, n=n), name="scatter", out_shape=_like(rows, columns), in_specs=[pl.BlockSpec(memory_space=pl.ANY)],
        out_specs=pl.BlockSpec(memory_space=pltpu.VMEM),
        scratch_shapes=[slots(c) for c in (chips, chips, far[0], far[0], far[1], far[1])]
        + [pltpu.SemaphoreType.DMA((chips,)), sems(chips), sems(far[0]), sems(far[1])],
        compiler_params=pltpu.CompilerParams(collective_id=1, has_side_effects=True))(x)


def _clip(*refs, n):
    *piece, out_ref, tile, held, sems = refs
    me = lax.axis_index("dp")
    others = [lax.rem(me + k, n) for k in range(1, n)]
    _greet(others)
    squares, count = jnp.zeros((1, 1), F32), 0
    for p in piece:
        count += n * p.shape[0] * p.shape[1]
        squares = squares + jnp.sum(jnp.square(p[...].astype(F32)), keepdims=True)
    tile[...] = jnp.broadcast_to(squares, tile.shape)
    out = [_send(tile, held.at[k], sems, k, other) for k, other in enumerate(others)]
    for one in out:
        one.start()
    for one in out:
        one.wait()
    total = tile[...]
    for k in range(n - 1):
        total = total + held[k]
    out_ref[...] = jnp.minimum(1.0, 0.5 * lax.rsqrt(total / count + 1e-30))


def _adamw(factor_ref, *refs, places, pieces):
    names, per = len(NAMES), 3 * len(NAMES)
    piece, given, made, bufs = (refs[a : a + c] for a, c in ((0, pieces), (pieces, per), (pieces + per, per), (pieces + 2 * per, per)))
    in_sem, out_sem = refs[pieces + 3 * per :]
    load = [pltpu.make_async_copy(a, b, in_sem.at[i]) for i, (a, b) in enumerate(zip(given, bufs))]
    for at in range(names):
        for one in load[at::names]:
            one.start()
    factor = factor_ref[0:1, 0:1]
    stored = []
    for at, name in enumerate(NAMES):
        w_ref, m_ref, v_ref = trio = bufs[at::names]
        for one in load[at::names]:
            one.wait()
        for i in range(w_ref.shape[0]):
            which, first = places[name][i]
            if name == "w_down":
                g = _down_read(piece[which][:, first : first + 16 * w_ref.shape[1]], w_ref.shape[2])
            else:
                g = piece[which][:, first : first + w_ref.shape[2]]
            g = g.astype(F32) * factor
            m = 0.9 * m_ref[i] + 0.1 * g
            v = 0.95 * v_ref[i] + 0.05 * g * g
            w = w_ref[i].astype(F32)
            w_ref[i] = (w - 0.02 * (m * lax.rsqrt(v + 1e-8) + 0.1 * w)).astype(BF)
            m_ref[i] = m
            v_ref[i] = v
        for a, b, k in zip(trio, made[at::names], range(at, per, names)):
            stored.append(pltpu.make_async_copy(a, b, out_sem.at[k]))
            stored[-1].start()
    for one in stored:
        one.wait()


def finished(pieces, arrays, places, n):
    vmem, anywhere = pl.BlockSpec(memory_space=pltpu.VMEM), pl.BlockSpec(memory_space=pl.ANY)
    small = pltpu.VMEM((8, HEAD), F32)
    count = len(arrays)
    factor = pl.pallas_call(
        functools.partial(_clip, n=n), name="clip", out_shape=_like(8, HEAD, dtype=F32), in_specs=[vmem] * len(pieces), out_specs=vmem,
        scratch_shapes=[small, pltpu.VMEM((n - 1, 8, HEAD), F32), pltpu.SemaphoreType.DMA((2, n - 1))],
        compiler_params=pltpu.CompilerParams(collective_id=2, has_side_effects=True))(*pieces)
    return pl.pallas_call(
        functools.partial(_adamw, places=places, pieces=len(pieces)), name="adamw", out_shape=[_like(*a.shape, dtype=a.dtype) for a in arrays],
        in_specs=[vmem] * (1 + len(pieces)) + [anywhere] * count, out_specs=[anywhere] * count,
        scratch_shapes=[pltpu.VMEM(a.shape, a.dtype) for a in arrays] + [pltpu.SemaphoreType.DMA((count,))] * 2,
        compiler_params=pltpu.CompilerParams(vmem_limit_bytes=VMEM))(factor, *pieces, *arrays)


def _price(flops, *arrays):
    return pl.CostEstimate(flops=int(flops), transcendentals=0, bytes_accessed=int(sum(a.size * a.dtype.itemsize for a in arrays)))


def _whole(shape):
    return pl.BlockSpec(shape, lambda *_: (0,) * len(shape))


def _like(*shape, dtype=BF):
    return jax.ShapeDtypeStruct(shape, dtype)


def solution(mesh):
    n = mesh.shape["dp"]

    def step(x, dy, *arrays):
        weights = dict(zip(NAMES, arrays[: len(NAMES)], strict=True))
        layers, ff, d = weights["wq"].shape[0], weights["w_gate"].shape[2], x.shape[2]
        tokens = x.shape[1]
        dq, kv = weights["wq"].shape[2], 2 * weights["wk"].shape[2]
        heads, u = dq // HEAD, ff // n
        mlp, att = 3 * ff, kv + d + dq
        tall = TILE // u * (d // 16)
        keep = _params()
        anywhere = pl.BlockSpec(memory_space=pl.ANY)

        angle = jnp.arange(tokens, dtype=F32)[:, None] * THETA ** (-jnp.arange(HEAD // 2, dtype=F32) / (HEAD // 2))
        cos, sin = jnp.cos(angle), jnp.sin(angle)
        c, s = jnp.concatenate([cos, cos], 1), jnp.concatenate([-sin, sin], 1)

        beside = lambda names, i: jnp.concatenate([weights[name][i] for name in names], 1)
        around = gathered([beside(("wo", "wq", "wk", "wv"), i) for i in range(layers)], n)
        middle = [lax.all_gather(jnp.concatenate([beside(("w_gate", "w_up"), i), packed_down(weights["w_down"][i])], 1), "dp", axis=0, tiled=True)
                  for i in range(layers)]

        w_o, w_q, w_kv = (pl.BlockSpec((d, width), lambda *_, at=start // width: (0, at)) for width, start in ((d, 0), (dq, d), (kv, d + dq)))
        w_gate = pl.BlockSpec((d, TILE), lambda j: (0, j))
        w_up = pl.BlockSpec((d, TILE), lambda j: (0, ff // TILE + j))
        w_down = pl.BlockSpec((tall, ff), lambda j: (j, 2))

        def qkv(h, w):
            rows = 256
            block = lambda width: pl.BlockSpec((rows, width), lambda j: (j, 0))
            return pl.pallas_call(
                _qkv, name="qkv", grid=(tokens // rows,), in_specs=[block(d), w_kv, w_q, block(HEAD), block(HEAD)],
                out_specs=[pl.BlockSpec((heads, rows, HEAD), lambda j: (0, j, 0)), block(HEAD), block(HEAD)],
                out_shape=[_like(heads, tokens, HEAD), _like(tokens, HEAD), _like(tokens, HEAD)], compiler_params=keep,
                cost_estimate=_price(2 * tokens * d * (dq + kv), h, h, h))(h, w, w, c, s)

        def through_mlp(h, o, a, w):
            return pl.pallas_call(
                _mlp, name="mlp", grid=(ff // TILE,),
                in_specs=[_whole(h.shape), _whole(o.shape), w_o, w_gate, w_up, w_down],
                out_specs=[_whole(h.shape), _whole(h.shape)], out_shape=[_like(*h.shape), _like(*h.shape)],
                scratch_shapes=[pltpu.VMEM(h.shape, BF), pltpu.VMEM(h.shape, F32), pltpu.VMEM((tokens, TILE), BF), pltpu.VMEM((TILE, d), BF)],
                compiler_params=keep,
                cost_estimate=_price(2 * tokens * d * (mlp + d), h, h, h, w))(h, o, a, w, w, w)

        def mlp_back(mid, dh, o, a, w, into):
            given = [mid, dh, o, a, w, w, w, jnp.ones((8, HEAD), F32)]
            specs = [_whole(mid.shape), _whole(mid.shape), _whole(o.shape), w_o, w_gate, w_up, w_down, _whole((8, HEAD))]
            out = _like(d, mlp) if into is None else into
            wide = pltpu.VMEM((tokens, TILE), BF)
            return pl.pallas_call(
                functools.partial(_mlp_back, aliased=into is not None), name="mlp_back", grid=(ff // TILE,),
                in_specs=specs + ([] if into is None else [anywhere]),
                out_specs=[_whole(mid.shape), _whole(o.shape), _whole((heads, tokens)), anywhere],
                out_shape=[_like(*mid.shape), _like(*o.shape), _like(heads, tokens, dtype=F32), _like(*out.shape)],
                input_output_aliases={} if into is None else {8: 3},
                scratch_shapes=[pltpu.VMEM(mid.shape, BF), pltpu.VMEM(mid.shape, F32), wide, wide, wide, pltpu.VMEM((TILE, d), BF),
                                pltpu.VMEM((d, TILE), BF), pltpu.VMEM((d, TILE), BF), pltpu.VMEM((tall, ff), BF),
                                pltpu.SemaphoreType.DMA((3,))],
                compiler_params=keep, cost_estimate=_price(2 * tokens * d * (8 * ff + d), mid, mid, mid, w, w),
            )(*given, *([] if into is None else [into]))

        def qkv_back(parts, h, dmid, o, w, at, columns, deeper):
            given = [*parts, c, s, h, dmid, o, w, w]
            specs = [_whole(a.shape) for a in given[:-2]] + [w_kv, w_q]
            out = _like(d, columns)
            got = pl.pallas_call(
                functools.partial(_qkv_back, at=at, deeper=deeper), name="qkv_back", grid=(1,),
                in_specs=specs, out_specs=([_whole(h.shape)] if deeper else []) + [anywhere],
                out_shape=([_like(*h.shape)] if deeper else []) + [out],
                scratch_shapes=[pltpu.VMEM(h.shape, BF), pltpu.VMEM((tokens, dq), BF), pltpu.VMEM((tokens, kv), BF),
                                pltpu.VMEM((d, att), BF), pltpu.SemaphoreType.DMA],
                compiler_params=keep, cost_estimate=_price(4 * tokens * d * att, h, h, h, h, h))(*given)
            return got if deeper else [None, got[0]]

        h, kept = x[0], []
        for i in range(layers):
            q, k, v = qkv(h, around[i])
            o, lse = attend(q, k, v)
            mid, after = through_mlp(h, o, around[i], middle[i])
            kept.append((h, q, k, v, o, lse, mid))
            h = after

        dh, into, pieces = dy[0], None, [None] * layers
        for i in reversed(range(layers)):
            h, q, k, v, o, lse, mid = kept[i]
            dmid, do, delta, into = mlp_back(mid, dh, o, around[i], middle[i], into)
            pieces[i] = lax.psum_scatter(into, "dp", scatter_dimension=0, tiled=True)
            parts = attend_bwd(q, k, v, do, lse, delta)
            dh, into = qkv_back(parts, h, dmid, o, around[i], mlp if i else 0, mlp + att if i else att, i > 0)
        pieces.append(scattered(into, n))

        places = {name: [(i, at) for i in range(layers)] for name, at in (("w_gate", 0), ("w_up", ff), ("w_down", 2 * ff))}
        for name, at in (("wo", 0), ("wq", d), ("wk", d + dq), ("wv", d + dq + kv // 2)):
            places[name] = [(i - 1, mlp + at) if i else (layers, at) for i in range(layers)]
        return tuple(finished(pieces, arrays, places, n))

    states, cut = P(("rep", "dp"), None, None), P(None, "dp", None)
    return jax.shard_map(
        step,
        mesh=mesh,
        in_specs=(states, states) + (cut,) * 21,
        out_specs=(P("rep", "dp", None),) * 21,
        check_vma=False,
    )
```
